32 devices in a mesh: row: 4 (over z), col: 8 (over y, x, core).
Axes of the slice: x: 2, y: 2, z: 4, core: 2. Of those that a mesh axis runs over, the one named last changes fastest.
Arguments:
- v_panels: float32 [8192, 8192], P('row', 'col')
- t_factors: float32 [128, 64, 64], P('col')
- z_vecs: float32 [8192, 1024], P(None, ('row', 'col'))
Outputs:
- output: float32 [8192, 1024], P(None, ('row', 'col'))
All inputs are finite; a program needn't handle non-finite values.
Results may differ from the reference program's by a relative error of at most 0.001.
Values sent between devices are 32-bit elements.
A program may use at most 1 GiB of HBM per device.

```python
import jax
import jax.numpy as jnp
from jax import lax

N = 8192
BLOCK = 64
K_DEV = 32
ROW_DEV = 4
COL_DEV = 8

NPANEL = N // BLOCK
M_LOC = NPANEL // COL_DEV
K_COLS = K_DEV * ROW_DEV * COL_DEV


def build_inputs(raw_vals, z_vecs):
    row_nat = jnp.arange(N)[:, None, None]
    diag_row = (jnp.arange(NPANEL) * BLOCK)[None, :, None] + jnp.arange(BLOCK)[None, None, :]
    v_nat = jnp.where(row_nat > diag_row, raw_vals, jnp.where(row_nat == diag_row, 1.0, 0.0)).astype(raw_vals.dtype)
    gram = jnp.einsum("nmb,nmc->mbc", v_nat, v_nat, precision=lax.Precision.HIGHEST)
    half_diag = 0.5 * jnp.diagonal(gram, axis1=1, axis2=2)
    t_inverse = jnp.triu(gram, 1) + jnp.eye(BLOCK, dtype=raw_vals.dtype) * half_diag[:, None, :]
    t_nat = jnp.triu(jnp.linalg.inv(t_inverse))
    v_cols = v_nat.reshape(N, M_LOC, COL_DEV, BLOCK).transpose(0, 2, 1, 3).reshape(N, N)
    v_store = v_cols.reshape(NPANEL // ROW_DEV, ROW_DEV, BLOCK, N).transpose(1, 0, 2, 3).reshape(N, N)
    t_store = t_nat.reshape(M_LOC, COL_DEV, BLOCK, BLOCK).transpose(1, 0, 2, 3).reshape(NPANEL, BLOCK, BLOCK)
    return {"v_panels": v_store, "t_factors": t_store, "z_vecs": z_vecs}


def setup_inputs(seed: int = 0) -> dict:
    base_key = jax.random.key(seed)
    key_v, key_z = jax.random.split(base_key)
    raw_vals = jax.random.normal(key_v, (N, NPANEL, BLOCK), jnp.float32)
    z_vecs = jax.random.normal(key_z, (N, K_COLS), jnp.float32)
    return build_inputs(raw_vals, z_vecs)


def reference(v_panels, t_factors, z_vecs):
    def apply_panel(x_cur, panel_idx):
        store_slot = (panel_idx % COL_DEV) * M_LOC + panel_idx // COL_DEV
        v_blk = lax.dynamic_slice_in_dim(v_panels, store_slot * BLOCK, BLOCK, axis=1)
        t_blk = lax.dynamic_index_in_dim(t_factors, store_slot, axis=0, keepdims=False)
        w_blk = jnp.dot(v_blk.T, x_cur, precision=lax.Precision.HIGHEST, preferred_element_type=jnp.float32)
        y_blk = jnp.dot(t_blk, w_blk, precision=lax.Precision.HIGHEST, preferred_element_type=jnp.float32)
        x_new = x_cur - jnp.dot(v_blk, y_blk, precision=lax.Precision.HIGHEST, preferred_element_type=jnp.float32)
        return x_new, None

    x_out, _ = lax.scan(apply_panel, z_vecs, jnp.arange(NPANEL - 1, -1, -1))
    return x_out
```

```python
import jax
import jax.numpy as jnp
from jax import lax
from jax.sharding import PartitionSpec as P

HI = lax.Precision.HIGHEST
F32 = jnp.float32


def mm(a, b, ca, cb):
    return lax.dot_general(a, b, (((ca,), (cb,)), ((), ())), precision=HI, preferred_element_type=F32)


def bmm(a, b):
    return jnp.matmul(a, b, precision=HI, preferred_element_type=F32)


def solution(mesh):
    nc = mesh.shape["col"]

    def body(v_loc, t_loc, z_loc):
        nt, bw = t_loc.shape[0], t_loc.shape[1]
        ng = nt // 2
        gw = 2 * bw * nc
        rows = v_loc.shape[0]
        rstep = rows // ng
        x = lax.all_to_all(z_loc, "row", 0, 1, tiled=True)
        t_all = lax.all_gather(t_loc, "col")
        vgs, slabs = {}, []
        for a in range(ng - 1, -1, -1):
            vb = lax.slice(v_loc, (a * rstep, a * 2 * bw), (rows, (a + 1) * 2 * bw))
            vg = lax.all_gather(vb, "col", axis=1, tiled=True)
            vgs[a] = vg
            slabs.append(mm(vg, vb, 0, 0))
        slab = lax.psum(jnp.stack(slabs[::-1]), "row")
        gram = lax.all_gather(slab, "col")
        gram = gram.reshape(nc, ng, nc, 2, bw, 2, bw).transpose(1, 3, 2, 4, 5, 0, 6).reshape(ng, gw, gw)
        cur = t_all.reshape(nc, ng, 2, bw, bw).transpose(1, 2, 0, 3, 4)
        cur = cur.reshape(ng, 2 * nc, bw, bw)
        size, cnt = bw, 2 * nc
        while cnt > 1:
            half = cnt // 2
            g01 = jnp.stack([gram[:, (2 * i) * size:(2 * i + 1) * size, (2 * i + 1) * size:(2 * i + 2) * size]
                             for i in range(half)], axis=1)
            t0, t1 = cur[:, 0::2], cur[:, 1::2]
            t01 = -bmm(t0, bmm(g01, t1))
            top = jnp.concatenate([t0, t01], axis=-1)
            bot = jnp.concatenate([jnp.zeros_like(t01), t1], axis=-1)
            cur = jnp.concatenate([top, bot], axis=-2)
            size, cnt = 2 * size, half
        big = cur[:, 0]
        big = big.reshape(ng, 2, nc, bw, 2, nc, bw).transpose(0, 2, 1, 3, 5, 4, 6).reshape(ng, gw, gw)
        for a in range(ng - 1, -1, -1):
            xs = x[a * rstep:]
            w = lax.psum(mm(vgs[a], xs, 0, 0), "row")
            y = mm(big[a], w, 1, 0)
            xs = xs - mm(vgs[a], y, 1, 0)
            x = jnp.concatenate([x[:a * rstep], xs], axis=0)
        return lax.all_to_all(x, "row", 1, 0, tiled=True)

    return jax.shard_map(
        body,
        mesh=mesh,
        in_specs=(P("row", "col"), P("col", None, None), P(None, ("row", "col"))),
        out_specs=P(None, ("row", "col")),
        check_vma=False,
    )
```

```python
import functools

import jax
import jax.numpy as jnp
from jax import lax
from jax.experimental import pallas as pl
from jax.experimental.pallas import tpu as pltpu
from jax.sharding import PartitionSpec as P

F32 = jnp.float32
HI = lax.Precision.HIGHEST
MESH = pl.DeviceIdType.MESH
TR = 256


def dot(a, b, ca, cb):
    return lax.dot_general(a, b, (((ca,), (cb,)), ((), ())), precision=HI, preferred_element_type=F32)


def kernel(na, v_ref, tl_ref, zt_ref, out_ref, vbuf, tbuf, xt, vn, tc, gacc, tm, wp, wrs, ybuf, gpart, grs, gbuf,
           lsem, vsend, vrecv, tsend, trecv, fsend, tfsend, zsend, zrecv, osend, orecv,
           wsend, wrecv, ysend, yrecv, gsend, grecv, hsend, hrecv):
    rr = lax.axis_index("row")
    c = lax.axis_index("col")
    rloc = TR * na
    nsteps = 4 * na
    core, cx, cy = c % 2, (c // 2) % 2, c // 4
    mate = c + 1 - 2 * core
    xn = c + 2 - 4 * cx
    yn = c + 4 - 8 * cy
    dg = yn + 2 - 4 * cx
    same = (xn, yn, dg)

    def zpeer(d):
        return lax.rem(rr + d, 4)

    barrier = pltpu.get_barrier_semaphore()
    for p in (mate, xn, yn, dg):
        pl.semaphore_signal(barrier, inc=1, device_id=(rr, p), device_id_type=MESH)
    for d in (1, 2, 3):
        pl.semaphore_signal(barrier, inc=1, device_id=(zpeer(d), c), device_id_type=MESH)
    pl.semaphore_wait(barrier, 7)

    def rows(a):
        return pl.ds(128 * (na - 1 - a) * (na - a), rloc - TR * a)

    def vdst(q, a):
        return vbuf.at[q, rows(a), :]

    def rc(src, dst, ss, rs, dev):
        return pltpu.make_async_remote_copy(src_ref=src, dst_ref=dst, send_sem=ss, recv_sem=rs,
                                            device_id=dev, device_id_type=MESH)

    def vsrc(a):
        return v_ref.at[pl.ds(TR * a, rloc - TR * a), pl.ds(128 * a, 128)]

    def tsrc(a):
        return tl_ref.at[:, pl.ds(128 * a, 128)]

    def locals_(a):
        return (pltpu.make_async_copy(vsrc(a), vdst(c, a), lsem.at[0, a]),
                pltpu.make_async_copy(tsrc(a), tbuf.at[c, a], lsem.at[1, a]))

    def sends(a):
        out = []
        for n, p in enumerate((xn, yn, dg, mate)):
            out.append(rc(tsrc(a), tbuf.at[c, a], tsend.at[a, n], trecv.at[a, c], (rr, p)))
            out.append(rc(vsrc(a), vdst(c, a), vsend.at[a, n], vrecv.at[a, c], (rr, p)))
        return out

    def forwards(a):
        out = []
        for n, q in enumerate(same):
            out.append(rc(tbuf.at[q, a], tbuf.at[q, a], tfsend.at[a, n], trecv.at[a, q], (rr, mate)))
            out.append(rc(vdst(q, a), vdst(q, a), fsend.at[a, n], vrecv.at[a, q], (rr, mate)))
        return out

    def incoming(a, q):
        return (rc(tbuf.at[q, a], tbuf.at[q, a], tsend.at[a, 0], trecv.at[a, q], (rr, mate)),
                rc(vdst(q, a), vdst(q, a), vsend.at[a, 0], vrecv.at[a, q], (rr, mate)))

    def start_group(a):
        for cp in locals_(a):
            cp.start()
        for cp in sends(a):
            cp.start()

    def forward_group(a):
        for n, q in enumerate(same):
            for cp in incoming(a, q):
                cp.wait_recv()
        for cp in forwards(a):
            cp.start()

    def wait_group(a):
        for cp in locals_(a):
            cp.wait()
        for q in (mate, mate + xn - c, mate + yn - c, mate + dg - c):
            for cp in incoming(a, q):
                cp.wait_recv()

    zin = pltpu.make_async_copy(zt_ref.at[:, pl.ds(pl.multiple_of(rr * rloc, rloc), rloc)],
                                xt.at[pl.ds(pl.multiple_of(32 * rr, 32), 32), :], lsem.at[2, 0])
    zin.start()
    zcp = [rc(zt_ref.at[:, pl.ds(pl.multiple_of(zpeer(d) * rloc, rloc), rloc)],
              xt.at[pl.ds(pl.multiple_of(32 * rr, 32), 32), :],
              zsend.at[d - 1], zrecv.at[d - 1], (zpeer(d), c)) for d in (1, 2, 3)]
    for cp in zcp:
        cp.start()
    for a in range(na - 1, max(na - 4, -1), -1):
        start_group(a)

    lane = lax.broadcasted_iota(jnp.int32, (1, 128), 1)
    lo = lane < 64

    def deint(b, tt):
        first, second = [], []
        r = [pltpu.roll(x, 64, axis=1) for x in b]
        left0, right0 = jnp.where(lo, b[0], r[1]), jnp.where(lo, b[2], r[3])
        left1, right1 = jnp.where(lo, r[0], b[1]), jnp.where(lo, r[2], b[3])
        sel = tt == 0
        return jnp.concatenate([jnp.where(sel, left0, left1), jnp.where(sel, right0, right1)], axis=1)

    def prepare(i):
        a = na - 1 - i // 4
        tt = 1 - (i % 4) // 2
        h = 1 - i % 2
        slot = i % 2
        tc[slot] = deint([tbuf[4 * h + n, a] for n in range(4)], tt)
        gacc[...] = jnp.zeros_like(gacc)
        base = 128 * (na - 1 - a) * (na - a)

        def tile(t, _):
            src = pl.multiple_of(base + (t - a) * TR, 128)
            v = deint([vbuf[4 * h + n, pl.ds(src, TR), :] for n in range(4)], tt)
            vn[slot, pl.ds(pl.multiple_of(t * TR, TR), TR), :] = v
            gacc[...] += dot(v, v, 0, 0)
            return 0

        lax.fori_loop(a, na, tile, 0)
        gpart[0:128, :] = gacc[0:128, 128:256]
        gpart[128:192, :] = jnp.where(lo, pltpu.roll(gacc[0:64, 0:128], 64, axis=1), gacc[128:192, 128:256])

    def gcopies():
        return [rc(gpart.at[pl.ds(pl.multiple_of(48 * zpeer(d), 8), 48), :], grs.at[d - 1],
                   gsend.at[d - 1], grecv.at[d - 1], (zpeer(d), c)) for d in (1, 2, 3)]

    def hcopies(slot):
        mine = pl.ds(pl.multiple_of(48 * rr, 8), 48)
        return [rc(gbuf.at[slot, mine, :], gbuf.at[slot, mine, :],
                   hsend.at[d - 1], hrecv.at[d - 1], (zpeer(d), c)) for d in (1, 2, 3)]

    def gsum(slot):
        mine = pl.ds(pl.multiple_of(48 * rr, 8), 48)
        gbuf[slot, mine, :] = (gpart[mine, :] + grs[0]) + (grs[1] + grs[2])

    def form_t(slot):
        tcv = tc[slot]
        lane2 = lax.broadcasted_iota(jnp.int32, (1, 256), 1) // 64
        dm = jnp.concatenate([jnp.where(lane2 == n, tcv, 0.0) for n in range(4)], axis=0)
        pk = gbuf[slot, 128:192, :]
        z64 = jnp.zeros((64, 128), F32)
        z256 = jnp.zeros((64, 256), F32)
        n1 = jnp.concatenate([jnp.concatenate([jnp.where(lo, 0.0, pltpu.roll(pk, 64, axis=1)), z64], axis=1), z256,
                              jnp.concatenate([z64, jnp.where(lo, 0.0, pk)], axis=1), z256], axis=0)
        tm[...] = dm - dot(dm, dot(n1, dm, 1, 0), 1, 0)
        ta, tb = tm[0:128, 0:128], tm[128:256, 128:256]
        tm[0:128, 128:256] = -dot(ta, dot(gbuf[slot, 0:128, :], tb, 1, 0), 1, 0)

    forward_group(na - 1)
    wait_group(na - 1)
    prepare(0)
    for cp in gcopies():
        cp.start()
    for cp in gcopies():
        cp.wait_recv()
    gsum(0)
    for cp in hcopies(0):
        cp.start()
    zin.wait()
    for cp in zcp:
        cp.wait_recv()
    for cp in hcopies(0):
        cp.wait_recv()
    for cp in gcopies() + hcopies(0):
        cp.wait_send()

    def step(i, _):
        a = na - 1 - i // 4
        slot = i % 2
        nslot = 1 - slot
        for sa in range(na - 1, -1, -1):
            @pl.when(i == 4 * (na - 1 - sa))
            def _():
                if sa >= 1:
                    forward_group(sa - 1)
                if sa >= 4 - 1 and sa - 3 <= na - 4:
                    start_group(sa - 3)

        wp[...] = jnp.zeros_like(wp)

        def wtile(t, _):
            o = pl.multiple_of(t * TR, TR)
            wp[...] += dot(xt[:, pl.ds(o, TR)], vn[slot, pl.ds(o, TR), :], 1, 0)
            return 0

        lax.fori_loop(a, na, wtile, 0)
        wcp = [rc(wp.at[pl.ds(pl.multiple_of(32 * zpeer(d), 32), 32), :], wrs.at[d - 1],
                  wsend.at[d - 1], wrecv.at[d - 1], (zpeer(d), c)) for d in (1, 2, 3)]
        for cp in wcp:
            cp.start()

        @pl.when(i < nsteps - 1)
        def _():
            for sa in range(na - 2, -1, -1):
                @pl.when(i == 4 * (na - 1 - sa) - 1)
                def _():
                    wait_group(sa)
            prepare(i + 1)
            for cp in gcopies():
                cp.start()

        form_t(slot)
        mine = pl.ds(pl.multiple_of(32 * rr, 32), 32)
        for cp in wcp:
            cp.wait_recv()
        ybuf[mine, :] = dot((wp[mine, :] + wrs[0]) + (wrs[1] + wrs[2]), tm[...], 1, 1)
        ycp = [rc(ybuf.at[mine, :], ybuf.at[mine, :], ysend.at[d - 1], yrecv.at[d - 1], (zpeer(d), c))
               for d in (1, 2, 3)]
        for cp in ycp:
            cp.start()

        @pl.when(i < nsteps - 1)
        def _():
            for cp in gcopies():
                cp.wait_recv()
            gsum(nslot)
            for cp in hcopies(nslot):
                cp.start()

        for cp in ycp:
            cp.wait_recv()

        def utile(t, _):
            o = pl.multiple_of(t * TR, TR)
            xt[:, pl.ds(o, TR)] = xt[:, pl.ds(o, TR)] - dot(ybuf[...], vn[slot, pl.ds(o, TR), :], 1, 1)
            return 0

        lax.fori_loop(a, na, utile, 0)
        for cp in wcp + ycp:
            cp.wait_send()

        @pl.when(i < nsteps - 1)
        def _():
            for cp in hcopies(nslot):
                cp.wait_recv()
            for cp in gcopies() + hcopies(nslot):
                cp.wait_send()

        return 0

    lax.fori_loop(0, nsteps, step, 0)

    oloc = pltpu.make_async_copy(xt.at[pl.ds(pl.multiple_of(32 * rr, 32), 32), :],
                                 out_ref.at[:, pl.ds(pl.multiple_of(rr * rloc, rloc), rloc)], lsem.at[2, 0])
    oloc.start()
    ocp = [rc(xt.at[pl.ds(pl.multiple_of(32 * zpeer(d), 32), 32), :],
              out_ref.at[:, pl.ds(pl.multiple_of(rr * rloc, rloc), rloc)],
              osend.at[d - 1], orecv.at[d - 1], (zpeer(d), c)) for d in (1, 2, 3)]
    for cp in ocp:
        cp.start()
    for a in range(na - 1, -1, -1):
        for cp in sends(a) + forwards(a):
            cp.wait_send()
    for cp in zcp:
        cp.wait_send()
    oloc.wait()
    for cp in ocp:
        cp.wait()


def solution(mesh):
    def body(v_loc, t_loc, z_loc):
        nt, bw = t_loc.shape[0], t_loc.shape[1]
        na = nt // 2
        rloc = v_loc.shape[0]
        tl = t_loc.transpose(1, 0, 2).reshape(bw, nt * bw)
        zt = z_loc.T
        dma = pltpu.SemaphoreType.DMA
        tot = 128 * na * (na + 1)
        anyspec = pl.BlockSpec(memory_space=pl.ANY)
        out = pl.pallas_call(
            functools.partial(kernel, na),
            out_shape=jax.ShapeDtypeStruct(zt.shape, F32),
            in_specs=[anyspec] * 3,
            out_specs=anyspec,
            scratch_shapes=[
                pltpu.VMEM((8, tot, 128), F32),
                pltpu.VMEM((8, na, 64, 128), F32),
                pltpu.VMEM((128, rloc), F32),
                pltpu.VMEM((2, rloc, 256), F32),
                pltpu.VMEM((2, 64, 256), F32),
                pltpu.VMEM((256, 256), F32),
                pltpu.VMEM((256, 256), F32),
                pltpu.VMEM((128, 256), F32),
                pltpu.VMEM((3, 32, 256), F32),
                pltpu.VMEM((128, 256), F32),
                pltpu.VMEM((192, 128), F32),
                pltpu.VMEM((3, 48, 128), F32),
                pltpu.VMEM((2, 192, 128), F32),
                dma((3, na)),
                dma((na, 4)), dma((na, 8)), dma((na, 4)), dma((na, 8)), dma((na, 3)), dma((na, 3)),
                dma((3,)), dma((3,)), dma((3,)), dma((3,)),
                dma((3,)), dma((3,)), dma((3,)), dma((3,)), dma((3,)), dma((3,)), dma((3,)), dma((3,)),
            ],
            compiler_params=pltpu.CompilerParams(
                collective_id=0, has_side_effects=True, vmem_limit_bytes=60 * 2**20),
        )(v_loc, tl, zt)
        return out.T

    return jax.shard_map(
        body,
        mesh=mesh,
        in_specs=(P("row", "col"), P("col", None, None), P(None, ("row", "col"))),
        out_specs=P(None, ("row", "col")),
        check_vma=False,
    )
```

```python
import functools

import jax
import jax.numpy as jnp
from jax import lax
from jax.experimental import pallas as pl
from jax.experimental.pallas import tpu as pltpu
from jax.sharding import PartitionSpec as P

F32 = jnp.float32
HI = lax.Precision.HIGHEST
MESH = pl.DeviceIdType.MESH
TR = 256


def dot(a, b, ca, cb):
    return lax.dot_general(a, b, (((ca,), (cb,)), ((), ())), precision=HI, preferred_element_type=F32)


def kernel(na, v_ref, tl_ref, zt_ref, out_ref, vbuf, tbuf, xt, vn, tc, tm, wp, wrs, ybuf, gpart, grs, gbuf,
           lsem, zlsem, vsend, vrecv, tsend, trecv, fsend, tfsend, zsend, zrecv, osend, orecv,
           wsend, wrecv, ysend, yrecv, gsend, grecv, hsend, hrecv, psend, precv, pfsend):
    rr = lax.axis_index("row")
    c = lax.axis_index("col")
    rloc = TR * na
    nsteps = 2 * na
    core, cx, cy = c % 2, (c // 2) % 2, c // 4
    mate = c + 1 - 2 * core
    xn = c + 2 - 4 * cx
    yn = c + 4 - 8 * cy
    dg = yn + 2 - 4 * cx
    same = (xn, yn, dg)
    others = (mate, mate + xn - c, mate + yn - c, mate + dg - c)

    def zpeer(d):
        return lax.rem(rr + d, 4)

    def r16(r):
        return pl.ds(pl.multiple_of(16 * r, 16), 16)

    barrier = pltpu.get_barrier_semaphore()
    for p in (mate, xn, yn, dg):
        pl.semaphore_signal(barrier, inc=1, device_id=(rr, p), device_id_type=MESH)
    for d in (1, 2, 3):
        pl.semaphore_signal(barrier, inc=1, device_id=(zpeer(d), c), device_id_type=MESH)
    pl.semaphore_wait(barrier, 7)

    def rows(a):
        return pl.ds(128 * (na - 1 - a) * (na - a), rloc - TR * a)

    def vdst(q, a):
        return vbuf.at[q, rows(a), :]

    def rc(src, dst, ss, rs, dev):
        return pltpu.make_async_remote_copy(src_ref=src, dst_ref=dst, send_sem=ss, recv_sem=rs,
                                            device_id=dev, device_id_type=MESH)

    def vsrc(a):
        return v_ref.at[pl.ds(TR * a, rloc - TR * a), pl.ds(128 * a, 128)]

    def tsrc(a):
        return tl_ref.at[:, pl.ds(128 * a, 128)]

    def locals_(a):
        return (pltpu.make_async_copy(vsrc(a), vdst(c, a), lsem.at[0, a]),
                pltpu.make_async_copy(tsrc(a), tbuf.at[c, a], lsem.at[1, a]))

    def sends(a):
        out = []
        for n, p in enumerate((xn, yn, dg, mate)):
            out.append(rc(tsrc(a), tbuf.at[c, a], tsend.at[a, n], trecv.at[a, c], (rr, p)))
            out.append(rc(vsrc(a), vdst(c, a), vsend.at[a, n], vrecv.at[a, c], (rr, p)))
        return out

    def forwards(a):
        out = []
        for n, q in enumerate(same):
            out.append(rc(tbuf.at[q, a], tbuf.at[q, a], tfsend.at[a, n], trecv.at[a, q], (rr, mate)))
            out.append(rc(vdst(q, a), vdst(q, a), fsend.at[a, n], vrecv.at[a, q], (rr, mate)))
        return out

    def incoming(a, q):
        return (rc(tbuf.at[q, a], tbuf.at[q, a], tsend.at[a, 0], trecv.at[a, q], (rr, mate)),
                rc(vdst(q, a), vdst(q, a), vsend.at[a, 0], vrecv.at[a, q], (rr, mate)))

    def start_group(a):
        for cp in locals_(a):
            cp.start()
        for cp in sends(a):
            cp.start()

    def forward_group(a):
        for q in same:
            for cp in incoming(a, q):
                cp.wait_recv()
        for cp in forwards(a):
            cp.start()

    def wait_group(a):
        for cp in locals_(a):
            cp.wait()
        for q in others:
            for cp in incoming(a, q):
                cp.wait_recv()

    def mycols():
        return pl.ds(pl.multiple_of(rr * rloc, rloc), rloc)

    zin = [pltpu.make_async_copy(zt_ref.at[pl.ds(16 * p, 16), mycols()], xt.at[p, r16(rr), :], zlsem.at[p])
           for p in (0, 1)]
    zcp = [rc(zt_ref.at[pl.ds(16 * p, 16), pl.ds(pl.multiple_of(zpeer(d) * rloc, rloc), rloc)],
              xt.at[p, r16(rr), :], zsend.at[p, d - 1], zrecv.at[p, d - 1], (zpeer(d), c))
           for p in (0, 1) for d in (1, 2, 3)]
    start_group(na - 1)
    for cp in zin + zcp:
        cp.start()
    for a in range(na - 2, max(na - 5, -1), -1):
        start_group(a)

    lane = lax.broadcasted_iota(jnp.int32, (1, 128), 1)
    lo = lane < 64

    def deint(b, tt):
        sel = tt == 0
        out = []
        for n in range(0, 8, 2):
            lft = jnp.where(lo, b[n], pltpu.roll(b[n + 1], 64, axis=1))
            rgt = jnp.where(lo, pltpu.roll(b[n], 64, axis=1), b[n + 1])
            out.append(jnp.where(sel, lft, rgt))
        return jnp.concatenate(out, axis=1)

    def prepare(g):
        a = na - 1 - g // 2
        tt = 1 - g % 2
        slot = lax.rem(g, 3)
        tc[g % 2] = deint([tbuf[n, a] for n in range(8)], tt)
        gpart[...] = jnp.zeros_like(gpart)
        base = 128 * (na - 1 - a) * (na - a)

        def tile(t, _):
            src = pl.ds(pl.multiple_of(base + (t - a) * TR, 128), TR)
            v = deint([vbuf[n, src, :] for n in range(8)], tt)
            vn[slot, pl.ds(pl.multiple_of(t * TR, TR), TR), :] = v
            own = vbuf[c, src, :]
            own = jnp.where(tt == 0, own, pltpu.roll(own, 64, axis=1))[:, 0:64]
            gpart[...] += dot(own, v, 0, 0)
            return 0

        lax.fori_loop(a, na, tile, 0)

    def gcopies():
        return [rc(gpart.at[r16(zpeer(d)), :], grs.at[d - 1],
                   gsend.at[d - 1], grecv.at[d - 1], (zpeer(d), c)) for d in (1, 2, 3)]

    def gmine():
        return pl.ds(pl.multiple_of(64 * c + 16 * rr, 16), 16)

    def slab(q):
        return pl.ds(pl.multiple_of(64 * q, 64), 64)

    def hcopies(gs):
        return [rc(gbuf.at[gs, gmine(), :], gbuf.at[gs, gmine(), :],
                   hsend.at[d - 1], hrecv.at[d - 1], (zpeer(d), c)) for d in (1, 2, 3)]

    def pcopies(gs):
        return [rc(gbuf.at[gs, slab(c), :], gbuf.at[gs, slab(c), :], psend.at[n], precv.at[gs, c], (rr, p))
                for n, p in enumerate((xn, yn, dg, mate))]

    def pforwards(gs):
        return [rc(gbuf.at[gs, slab(q), :], gbuf.at[gs, slab(q), :], pfsend.at[n], precv.at[gs, q], (rr, mate))
                for n, q in enumerate(same)]

    def pin(gs, q):
        return rc(gbuf.at[gs, slab(q), :], gbuf.at[gs, slab(q), :], psend.at[0], precv.at[gs, q], (rr, mate))

    def gram_start():
        for cp in gcopies():
            cp.start()

    def gram_sum(gs):
        for cp in gcopies():
            cp.wait_recv()
        gbuf[gs, gmine(), :] = (gpart[r16(rr), :] + grs[0]) + (grs[1] + grs[2])
        for cp in hcopies(gs):
            cp.start()
        for cp in gcopies():
            cp.wait_send()

    def gram_plane(gs):
        for cp in hcopies(gs):
            cp.wait()
        for cp in pcopies(gs):
            cp.start()

    def gram_forward(gs):
        for q in same:
            pin(gs, q).wait_recv()
        for cp in pforwards(gs):
            cp.start()

    def gram_finish(gs):
        for q in others:
            pin(gs, q).wait_recv()
        for cp in pcopies(gs) + pforwards(gs):
            cp.wait_send()

    lane2 = lax.broadcasted_iota(jnp.int32, (1, 256), 1) // 64

    def form_t(gs):
        z256 = jnp.zeros((64, 256), F32)
        halves = []
        for o in (0, 256):
            tcv = tc[gs, :, o:o + 256]
            dm = jnp.concatenate([jnp.where(lane2 == n, tcv, 0.0) for n in range(4)], axis=0)
            n1 = jnp.concatenate([jnp.where(lane2 == 1, gbuf[gs, o:o + 64, o:o + 256], 0.0), z256,
                                  jnp.where(lane2 == 3, gbuf[gs, o + 128:o + 192, o:o + 256], 0.0), z256], axis=0)
            t1 = dm - dot(dm, dot(n1, dm, 1, 0), 1, 0)
            ta, tb = t1[0:128, 0:128], t1[128:256, 128:256]
            tx = -dot(ta, dot(gbuf[gs, o:o + 128, o + 128:o + 256], tb, 1, 0), 1, 0)
            top = jnp.concatenate([ta, tx], axis=1)
            bot = jnp.concatenate([jnp.zeros((128, 128), F32), tb], axis=1)
            halves.append(jnp.concatenate([top, bot], axis=0))
        tm[gs, 0] = halves[0].T
        tm[gs, 2] = halves[1].T
        tx = dot(halves[0], dot(gbuf[gs, 0:256, 256:512], halves[1], 1, 0), 1, 0)
        tm[gs, 1] = -(tx.T)

    def wcopies(p):
        return [rc(wp.at[p, r16(zpeer(d)), :], wrs.at[p, d - 1],
                   wsend.at[p, d - 1], wrecv.at[p, d - 1], (zpeer(d), c)) for d in (1, 2, 3)]

    def ycopies(p):
        return [rc(ybuf.at[p, r16(rr), :], ybuf.at[p, r16(rr), :],
                   ysend.at[p, d - 1], yrecv.at[p, d - 1], (zpeer(d), c)) for d in (1, 2, 3)]

    def w_part(i, p):
        a = na - 1 - i // 2
        slot = lax.rem(i, 3)
        wp[p] = jnp.zeros((64, 512), F32)

        def wtile(t, _):
            o = pl.ds(pl.multiple_of(t * TR, TR), TR)
            wp[p] += dot(xt[p, :, o], vn[slot, o, :], 1, 0)
            return 0

        lax.fori_loop(a, na, wtile, 0)
        for cp in wcopies(p):
            cp.start()

    def y_part(i, p):
        for cp in wcopies(p):
            cp.wait_recv()
        w = (wp[p, r16(rr), :] + wrs[p, 0]) + (wrs[p, 1] + wrs[p, 2])
        ts = i % 2
        wa, wb = w[:, 0:256], w[:, 256:512]
        ybuf[p, r16(rr), 0:256] = dot(wa, tm[ts, 0], 1, 0) + dot(wb, tm[ts, 1], 1, 0)
        ybuf[p, r16(rr), 256:512] = dot(wb, tm[ts, 2], 1, 0)
        for cp in ycopies(p):
            cp.start()
        for cp in wcopies(p):
            cp.wait_send()

    def x_part(i, p):
        a = na - 1 - i // 2
        slot = lax.rem(i, 3)
        for cp in ycopies(p):
            cp.wait_recv()

        def utile(t, _):
            o = pl.ds(pl.multiple_of(t * TR, TR), TR)
            xt[p, :, o] = xt[p, :, o] - dot(ybuf[p], vn[slot, o, :], 1, 1)
            return 0

        lax.fori_loop(a, na, utile, 0)
        for cp in ycopies(p):
            cp.wait_send()

    forward_group(na - 1)
    wait_group(na - 1)
    prepare(0)
    gram_start()
    gram_sum(0)
    gram_plane(0)
    prepare(1)
    gram_start()
    for cp in zin:
        cp.wait()
    for cp in zcp:
        cp.wait_recv()
    gram_forward(0)
    gram_finish(0)
    form_t(0)
    gram_sum(1)
    if na >= 2:
        forward_group(na - 2)
    if na >= 5:
        start_group(na - 5)

    def step(i, _):
        for sa in range(na - 3, -1, -1):
            @pl.when(i == 2 * (na - 1 - sa) - 3)
            def _():
                forward_group(sa)
                if sa >= 3:
                    start_group(sa - 3)

        ns = (i + 1) % 2
        w_part(i, 0)

        @pl.when(i < nsteps - 1)
        def _():
            gram_plane(ns)

        @pl.when(i > 0)
        def _():
            x_part(i - 1, 1)

        w_part(i, 1)
        y_part(i, 0)

        @pl.when(i < nsteps - 1)
        def _():
            gram_forward(ns)

        for sa in range(na - 2, -1, -1):
            @pl.when(i == 2 * (na - 1 - sa) - 2)
            def _():
                wait_group(sa)

        @pl.when(i < nsteps - 2)
        def _():
            prepare(i + 2)
            gram_start()

        y_part(i, 1)

        @pl.when(i < nsteps - 1)
        def _():
            gram_finish(ns)
            form_t(ns)

        x_part(i, 0)

        @pl.when(i < nsteps - 2)
        def _():
            gram_sum(i % 2)

        return 0

    lax.fori_loop(0, nsteps, step, 0)

    def outcopies(p):
        return [rc(xt.at[p, r16(zpeer(d)), :], out_ref.at[pl.ds(16 * p, 16), mycols()],
                   osend.at[p, d - 1], orecv.at[p, d - 1], (zpeer(d), c)) for d in (1, 2, 3)]

    oloc = [pltpu.make_async_copy(xt.at[p, r16(rr), :], out_ref.at[pl.ds(16 * p, 16), mycols()], zlsem.at[p])
            for p in (0, 1)]
    oloc[0].start()
    for cp in outcopies(0):
        cp.start()
    x_part(nsteps - 1, 1)
    oloc[1].start()
    for cp in outcopies(1):
        cp.start()
    for a in range(na - 1, -1, -1):
        for cp in sends(a) + forwards(a):
            cp.wait_send()
    for cp in zcp:
        cp.wait_send()
    for p in (0, 1):
        oloc[p].wait()
        for cp in outcopies(p):
            cp.wait()


def solution(mesh):
    def body(v_loc, t_loc, z_loc):
        nt, bw = t_loc.shape[0], t_loc.shape[1]
        na = nt // 2
        rloc = v_loc.shape[0]
        tl = t_loc.transpose(1, 0, 2).reshape(bw, nt * bw)
        zt = z_loc.T
        dma = pltpu.SemaphoreType.DMA
        tot = 128 * na * (na + 1)
        anyspec = pl.BlockSpec(memory_space=pl.ANY)
        out = pl.pallas_call(
            functools.partial(kernel, na),
            out_shape=jax.ShapeDtypeStruct(zt.shape, F32),
            in_specs=[anyspec] * 3,
            out_specs=anyspec,
            scratch_shapes=[
                pltpu.VMEM((8, tot, 128), F32),
                pltpu.VMEM((8, na, 64, 128), F32),
                pltpu.VMEM((2, 64, rloc), F32),
                pltpu.VMEM((3, rloc, 512), F32),
                pltpu.VMEM((2, 64, 512), F32),
                pltpu.VMEM((2, 3, 256, 256), F32),
                pltpu.VMEM((2, 64, 512), F32),
                pltpu.VMEM((2, 3, 16, 512), F32),
                pltpu.VMEM((2, 64, 512), F32),
                pltpu.VMEM((64, 512), F32),
                pltpu.VMEM((3, 16, 512), F32),
                pltpu.VMEM((2, 512, 512), F32),
                dma((2, na)), dma((2,)),
                dma((na, 4)), dma((na, 8)), dma((na, 4)), dma((na, 8)), dma((na, 3)), dma((na, 3)),
                dma((2, 3)), dma((2, 3)), dma((2, 3)), dma((2, 3)),
                dma((2, 3)), dma((2, 3)), dma((2, 3)), dma((2, 3)),
                dma((3,)), dma((3,)), dma((3,)), dma((3,)), dma((4,)), dma((2, 8)), dma((3,)),
            ],
            compiler_params=pltpu.CompilerParams(
                collective_id=0, has_side_effects=True, vmem_limit_bytes=67043328),
        )(v_loc, tl, zt)
        return out.T

    return jax.shard_map(
        body,
        mesh=mesh,
        in_specs=(P("row", "col"), P("col", None, None), P(None, ("row", "col"))),
        out_specs=P(None, ("row", "col")),
        check_vma=False,
    )
```

```python
import functools

import jax
import jax.numpy as jnp
from jax import lax
from jax.experimental import pallas as pl
from jax.experimental.pallas import tpu as pltpu
from jax.sharding import PartitionSpec as P

F32 = jnp.float32
HI = lax.Precision.HIGHEST
MESH = pl.DeviceIdType.MESH
TR = 256


def dot(a, b, ca, cb):
    return lax.dot_general(a, b, (((ca,), (cb,)), ((), ())), precision=HI, preferred_element_type=F32)


def kernel(na, v_ref, tl_ref, zt_ref, out_ref, vbuf, xt, vn, tc, tm, wp, wrs, ybuf, gpart, grs, gbuf,
           lsem, zlsem, vsend, vrecv, fsend, rsend, zsend, zrecv, osend, orecv,
           wsend, wrecv, ysend, yrecv, gsend, grecv, hsend, hrecv, psend, precv, pfsend):
    rr = lax.axis_index("row")
    c = lax.axis_index("col")
    rloc = TR * na
    nsteps = 2 * na
    core, cx, cy = c % 2, (c // 2) % 2, c // 4
    mate = c + 1 - 2 * core
    xn = c + 2 - 4 * cx
    yn = c + 4 - 8 * cy
    dg = yn + 2 - 4 * cx
    same = (xn, yn, dg)
    others = (mate, mate + xn - c, mate + yn - c, mate + dg - c)

    def zpeer(d):
        return lax.rem(rr + d, 4)

    def r16(r):
        return pl.ds(pl.multiple_of(16 * r, 16), 16)

    barrier = pltpu.get_barrier_semaphore()
    for p in (mate, xn, yn, dg):
        pl.semaphore_signal(barrier, inc=1, device_id=(rr, p), device_id_type=MESH)
    for d in (1, 2, 3):
        pl.semaphore_signal(barrier, inc=1, device_id=(zpeer(d), c), device_id_type=MESH)
    pl.semaphore_wait(barrier, 7)

    first = xn + core * (yn - xn)
    second = yn + core * (xn - yn)

    def base_of(a):
        return 128 * (na - 1 - a) * (na - a) + 64 * (na - 1 - a)

    def block(q, a):
        return vbuf.at[q, pl.ds(base_of(a), rloc - TR * a + 64), :]

    def rc(src, dst, ss, rs, dev):
        return pltpu.make_async_remote_copy(src_ref=src, dst_ref=dst, send_sem=ss, recv_sem=rs,
                                            device_id=dev, device_id_type=MESH)

    def locals_(a):
        n = rloc - TR * a
        return (pltpu.make_async_copy(tl_ref.at[:, pl.ds(128 * a, 128)],
                                      vbuf.at[c, pl.ds(base_of(a), 64), :], lsem.at[0, a]),
                pltpu.make_async_copy(v_ref.at[pl.ds(TR * a, n), pl.ds(128 * a, 128)],
                                      vbuf.at[c, pl.ds(base_of(a) + 64, n), :], lsem.at[1, a]))

    def move(q, a, sem, p):
        return rc(block(q, a), block(q, a), sem, vrecv.at[a, q], (rr, p))

    def sends(a):
        return [move(c, a, vsend.at[a, n], p) for n, p in enumerate((first, second, mate))]

    def near(a):
        return [move(first, a, rsend.at[a], second), move(first, a, fsend.at[a, 0], mate),
                move(second, a, fsend.at[a, 1], mate)]

    def far(a):
        return [move(dg, a, fsend.at[a, 2], mate)]

    def arrive(a, q):
        move(q, a, vsend.at[a, 0], mate).wait_recv()

    def stage1(a):
        for cp in locals_(a):
            cp.wait()
        for cp in sends(a):
            cp.start()

    def stage2(a):
        arrive(a, first)
        arrive(a, second)
        for cp in near(a):
            cp.start()

    def stage3(a):
        arrive(a, dg)
        for cp in far(a):
            cp.start()

    def stage4(a):
        for q in others:
            arrive(a, q)

    def mycols():
        return pl.ds(pl.multiple_of(rr * rloc, rloc), rloc)

    zin = [pltpu.make_async_copy(zt_ref.at[pl.ds(16 * p, 16), mycols()], xt.at[p, r16(rr), :], zlsem.at[p])
           for p in (0, 1)]
    zcp = [rc(zt_ref.at[pl.ds(16 * p, 16), pl.ds(pl.multiple_of(zpeer(d) * rloc, rloc), rloc)],
              xt.at[p, r16(rr), :], zsend.at[p, d - 1], zrecv.at[p, d - 1], (zpeer(d), c))
           for p in (0, 1) for d in (1, 2, 3)]
    for a in range(na - 1, -1, -1):
        for cp in locals_(a):
            cp.start()
    stage1(na - 1)
    for cp in zin + zcp:
        cp.start()
    for a in range(na - 2, max(na - 5, -1), -1):
        stage1(a)

    lane = lax.broadcasted_iota(jnp.int32, (1, 128), 1)
    lo = lane < 64

    def deint(b, tt):
        sel = tt == 0
        out = []
        for n in range(0, 8, 2):
            lft = jnp.where(lo, b[n], pltpu.roll(b[n + 1], 64, axis=1))
            rgt = jnp.where(lo, pltpu.roll(b[n], 64, axis=1), b[n + 1])
            out.append(jnp.where(sel, lft, rgt))
        return jnp.concatenate(out, axis=1)

    def prepare(g):
        a = na - 1 - g // 2
        tt = 1 - g % 2
        slot = lax.rem(g, 3)
        base = base_of(a)
        head = pl.ds(pl.multiple_of(base, 64), 64)
        tc[g % 2] = deint([vbuf[n, head, :] for n in range(8)], tt)
        gpart[...] = jnp.zeros_like(gpart)

        def tile(t, _):
            src = pl.ds(pl.multiple_of(base + 64 + (t - a) * TR, 64), TR)
            v = deint([vbuf[n, src, :] for n in range(8)], tt)
            vn[slot, pl.ds(pl.multiple_of(t * TR, TR), TR), :] = v
            own = vbuf[c, src, :]
            own = jnp.where(tt == 0, own, pltpu.roll(own, 64, axis=1))[:, 0:64]
            gpart[...] += dot(own, v, 0, 0)
            return 0

        lax.fori_loop(a, na, tile, 0)

    def gcopies():
        return [rc(gpart.at[r16(zpeer(d)), :], grs.at[d - 1],
                   gsend.at[d - 1], grecv.at[d - 1], (zpeer(d), c)) for d in (1, 2, 3)]

    def gmine():
        return pl.ds(pl.multiple_of(64 * c + 16 * rr, 16), 16)

    def slab(q):
        return pl.ds(pl.multiple_of(64 * q, 64), 64)

    def hcopies(gs):
        return [rc(gbuf.at[gs, gmine(), :], gbuf.at[gs, gmine(), :],
                   hsend.at[d - 1], hrecv.at[d - 1], (zpeer(d), c)) for d in (1, 2, 3)]

    def pcopies(gs):
        return [rc(gbuf.at[gs, slab(c), :], gbuf.at[gs, slab(c), :], psend.at[n], precv.at[gs, c], (rr, p))
                for n, p in enumerate((xn, yn, dg, mate))]

    def pforwards(gs):
        return [rc(gbuf.at[gs, slab(q), :], gbuf.at[gs, slab(q), :], pfsend.at[n], precv.at[gs, q], (rr, mate))
                for n, q in enumerate(same)]

    def pin(gs, q):
        return rc(gbuf.at[gs, slab(q), :], gbuf.at[gs, slab(q), :], psend.at[0], precv.at[gs, q], (rr, mate))

    def gram_start():
        for cp in gcopies():
            cp.start()

    def gram_sum(gs):
        for cp in gcopies():
            cp.wait_recv()
        gbuf[gs, gmine(), :] = (gpart[r16(rr), :] + grs[0]) + (grs[1] + grs[2])
        for cp in hcopies(gs):
            cp.start()
        for cp in gcopies():
            cp.wait_send()

    def gram_plane(gs):
        for cp in hcopies(gs):
            cp.wait()
        for cp in pcopies(gs):
            cp.start()

    def gram_forward(gs):
        for q in same:
            pin(gs, q).wait_recv()
        for cp in pforwards(gs):
            cp.start()

    def gram_finish(gs):
        for q in others:
            pin(gs, q).wait_recv()
        for cp in pcopies(gs) + pforwards(gs):
            cp.wait_send()

    lane2 = lax.broadcasted_iota(jnp.int32, (1, 256), 1) // 64

    def form_t(gs):
        z256 = jnp.zeros((64, 256), F32)
        halves = []
        for o in (0, 256):
            tcv = tc[gs, :, o:o + 256]
            dm = jnp.concatenate([jnp.where(lane2 == n, tcv, 0.0) for n in range(4)], axis=0)
            n1 = jnp.concatenate([jnp.where(lane2 == 1, gbuf[gs, o:o + 64, o:o + 256], 0.0), z256,
                                  jnp.where(lane2 == 3, gbuf[gs, o + 128:o + 192, o:o + 256], 0.0), z256], axis=0)
            t1 = dm - dot(dm, dot(n1, dm, 1, 0), 1, 0)
            ta, tb = t1[0:128, 0:128], t1[128:256, 128:256]
            tx = -dot(ta, dot(gbuf[gs, o:o + 128, o + 128:o + 256], tb, 1, 0), 1, 0)
            top = jnp.concatenate([ta, tx], axis=1)
            bot = jnp.concatenate([jnp.zeros((128, 128), F32), tb], axis=1)
            halves.append(jnp.concatenate([top, bot], axis=0))
        tm[gs, 0] = halves[0].T
        tm[gs, 2] = halves[1].T
        tx = dot(halves[0], dot(gbuf[gs, 0:256, 256:512], halves[1], 1, 0), 1, 0)
        tm[gs, 1] = -(tx.T)

    def wcopies(p):
        return [rc(wp.at[p, r16(zpeer(d)), :], wrs.at[p, d - 1],
                   wsend.at[p, d - 1], wrecv.at[p, d - 1], (zpeer(d), c)) for d in (1, 2, 3)]

    def ycopies(p):
        return [rc(ybuf.at[p, r16(rr), :], ybuf.at[p, r16(rr), :],
                   ysend.at[p, d - 1], yrecv.at[p, d - 1], (zpeer(d), c)) for d in (1, 2, 3)]

    def w_part(i, p):
        a = na - 1 - i // 2
        slot = lax.rem(i, 3)
        wp[p] = jnp.zeros((64, 512), F32)

        def wtile(t, _):
            o = pl.ds(pl.multiple_of(t * TR, TR), TR)
            wp[p] += dot(xt[p, :, o], vn[slot, o, :], 1, 0)
            return 0

        lax.fori_loop(a, na, wtile, 0)
        for cp in wcopies(p):
            cp.start()

    def y_part(i, p):
        for cp in wcopies(p):
            cp.wait_recv()
        w = (wp[p, r16(rr), :] + wrs[p, 0]) + (wrs[p, 1] + wrs[p, 2])
        ts = i % 2
        wa, wb = w[:, 0:256], w[:, 256:512]
        ybuf[p, r16(rr), 0:256] = dot(wa, tm[ts, 0], 1, 0) + dot(wb, tm[ts, 1], 1, 0)
        ybuf[p, r16(rr), 256:512] = dot(wb, tm[ts, 2], 1, 0)
        for cp in ycopies(p):
            cp.start()
        for cp in wcopies(p):
            cp.wait_send()

    def x_part(i, p):
        a = na - 1 - i // 2
        slot = lax.rem(i, 3)
        for cp in ycopies(p):
            cp.wait_recv()

        def utile(t, _):
            o = pl.ds(pl.multiple_of(t * TR, TR), TR)
            xt[p, :, o] = xt[p, :, o] - dot(ybuf[p], vn[slot, o, :], 1, 1)
            return 0

        lax.fori_loop(a, na, utile, 0)
        for cp in ycopies(p):
            cp.wait_send()

    stage2(na - 1)
    stage3(na - 1)
    stage4(na - 1)
    prepare(0)
    gram_start()
    gram_sum(0)
    gram_plane(0)
    prepare(1)
    gram_start()
    for cp in zin:
        cp.wait()
    for cp in zcp:
        cp.wait_recv()
    gram_forward(0)
    gram_finish(0)
    form_t(0)
    gram_sum(1)
    if na >= 2:
        stage2(na - 2)
        stage3(na - 2)

    def step(i, _):
        ns = (i + 1) % 2
        w_part(i, 0)

        @pl.when(i < nsteps - 1)
        def _():
            gram_plane(ns)

        for sa in range(na - 3, -1, -1):
            due = 2 * (na - 1 - sa) - 2

            @pl.when(i == due - 2)
            def _():
                stage2(sa)

            @pl.when(i == due - 1)
            def _():
                stage3(sa)

            if due >= 6:
                @pl.when(i == due - 5)
                def _():
                    stage1(sa)

        @pl.when(i > 0)
        def _():
            x_part(i - 1, 1)

        w_part(i, 1)
        y_part(i, 0)

        @pl.when(i < nsteps - 1)
        def _():
            gram_forward(ns)

        for sa in range(na - 2, -1, -1):
            @pl.when(i == 2 * (na - 1 - sa) - 2)
            def _():
                stage4(sa)

        @pl.when(i < nsteps - 2)
        def _():
            prepare(i + 2)
            gram_start()

        y_part(i, 1)

        @pl.when(i < nsteps - 1)
        def _():
            gram_finish(ns)
            form_t(ns)

        x_part(i, 0)

        @pl.when(i < nsteps - 2)
        def _():
            gram_sum(i % 2)

        return 0

    lax.fori_loop(0, nsteps, step, 0)

    def outcopies(p):
        return [rc(xt.at[p, r16(zpeer(d)), :], out_ref.at[pl.ds(16 * p, 16), mycols()],
                   osend.at[p, d - 1], orecv.at[p, d - 1], (zpeer(d), c)) for d in (1, 2, 3)]

    oloc = [pltpu.make_async_copy(xt.at[p, r16(rr), :], out_ref.at[pl.ds(16 * p, 16), mycols()], zlsem.at[p])
            for p in (0, 1)]
    oloc[0].start()
    for cp in outcopies(0):
        cp.start()
    x_part(nsteps - 1, 1)
    oloc[1].start()
    for cp in outcopies(1):
        cp.start()
    for a in range(na - 1, -1, -1):
        for cp in sends(a) + near(a) + far(a):
            cp.wait_send()
    for cp in zcp:
        cp.wait_send()
    for p in (0, 1):
        oloc[p].wait()
        for cp in outcopies(p):
            cp.wait()


def solution(mesh):
    def body(v_loc, t_loc, z_loc):
        nt, bw = t_loc.shape[0], t_loc.shape[1]
        na = nt // 2
        rloc = v_loc.shape[0]
        tl = t_loc.transpose(1, 0, 2).reshape(bw, nt * bw)
        zt = z_loc.T
        dma = pltpu.SemaphoreType.DMA
        tot = 128 * na * (na + 1) + 64 * na
        anyspec = pl.BlockSpec(memory_space=pl.ANY)
        out = pl.pallas_call(
            functools.partial(kernel, na),
            out_shape=jax.ShapeDtypeStruct(zt.shape, F32),
            in_specs=[anyspec] * 3,
            out_specs=anyspec,
            scratch_shapes=[
                pltpu.VMEM((8, tot, 128), F32),
                pltpu.VMEM((2, 64, rloc), F32),
                pltpu.VMEM((3, rloc, 512), F32),
                pltpu.VMEM((2, 64, 512), F32),
                pltpu.VMEM((2, 3, 256, 256), F32),
                pltpu.VMEM((2, 64, 512), F32),
                pltpu.VMEM((2, 3, 16, 512), F32),
                pltpu.VMEM((2, 64, 512), F32),
                pltpu.VMEM((64, 512), F32),
                pltpu.VMEM((3, 16, 512), F32),
                pltpu.VMEM((2, 512, 512), F32),
                dma((2, na)), dma((2,)),
                dma((na, 3)), dma((na, 8)), dma((na, 3)), dma((na,)),
                dma((2, 3)), dma((2, 3)), dma((2, 3)), dma((2, 3)),
                dma((2, 3)), dma((2, 3)), dma((2, 3)), dma((2, 3)),
                dma((3,)), dma((3,)), dma((3,)), dma((3,)), dma((4,)), dma((2, 8)), dma((3,)),
            ],
            compiler_params=pltpu.CompilerParams(
                collective_id=0, has_side_effects=True, vmem_limit_bytes=67043328),
        )(v_loc, tl, zt)
        return out.T

    return jax.shard_map(
        body,
        mesh=mesh,
        in_specs=(P("row", "col"), P("col", None, None), P(None, ("row", "col"))),
        out_specs=P(None, ("row", "col")),
        check_vma=False,
    )
```

```python
import functools

import jax
import jax.numpy as jnp
from jax import lax
from jax.experimental import pallas as pl
from jax.experimental.pallas import tpu as pltpu
from jax.sharding import PartitionSpec as P

F32 = jnp.float32
BF16 = jnp.bfloat16
HI = lax.Precision.HIGHEST
MESH = pl.DeviceIdType.MESH
TR = 256


def dot(a, b, ca, cb):
    return lax.dot_general(a, b, (((ca,), (cb,)), ((), ())), precision=HI, preferred_element_type=F32)


def split3(x):
    h = x.astype(BF16)
    r = x - h.astype(F32)
    m = r.astype(BF16)
    return h, m, (r - m.astype(F32)).astype(BF16)


def stack3(x):
    return jnp.concatenate(split3(x), axis=0)


def dot6(stack, parts, ca, cb):
    m = stack.shape[0] // 3
    dims = (((ca,), (cb,)), ((), ()))
    r1 = lax.dot_general(stack, parts[0], dims, preferred_element_type=F32)
    r2 = lax.dot_general(stack[0:2 * m], parts[1], dims, preferred_element_type=F32)
    r3 = lax.dot_general(stack[0:m], parts[2], dims, preferred_element_type=F32)
    return (((r1[2 * m:] + r3) + r2[m:]) + (r1[m:2 * m] + r2[0:m])) + r1[0:m]


def kernel(na, v_ref, tl_ref, zt_ref, out_ref, vbuf, xt, vnh, vnm, vnl, tmh, tmm, tml, th, wp, wrs, ybuf, ystk, gpart, grs, gbuf,
           lsem, zlsem, vsend, vrecv, fsend, rsend, zsend, zrecv, osend, orecv,
           wsend, wrecv, ysend, yrecv, gsend, grecv, hsend, hrecv, psend, precv, pfsend):
    rr = lax.axis_index("row")
    c = lax.axis_index("col")
    rloc = TR * na
    nsteps = 2 * na
    core, cx, cy = c % 2, (c // 2) % 2, c // 4
    mate = c + 1 - 2 * core
    xn = c + 2 - 4 * cx
    yn = c + 4 - 8 * cy
    dg = yn + 2 - 4 * cx
    same = (xn, yn, dg)
    others = (mate, mate + xn - c, mate + yn - c, mate + dg - c)

    def zpeer(d):
        return lax.rem(rr + d, 4)

    def r16(r):
        return pl.ds(pl.multiple_of(16 * r, 16), 16)

    barrier = pltpu.get_barrier_semaphore()
    for p in (mate, xn, yn, dg):
        pl.semaphore_signal(barrier, inc=1, device_id=(rr, p), device_id_type=MESH)
    for d in (1, 2, 3):
        pl.semaphore_signal(barrier, inc=1, device_id=(zpeer(d), c), device_id_type=MESH)
    pl.semaphore_wait(barrier, 7)

    first = xn + core * (yn - xn)
    second = yn + core * (xn - yn)

    def base_of(a):
        return 128 * (na - 1 - a) * (na - a) + 64 * (na - 1 - a)

    def block(q, a):
        return vbuf.at[q, pl.ds(base_of(a), rloc - TR * a + 64), :]

    def rc(src, dst, ss, rs, dev):
        return pltpu.make_async_remote_copy(src_ref=src, dst_ref=dst, send_sem=ss, recv_sem=rs,
                                            device_id=dev, device_id_type=MESH)

    def locals_(a):
        n = rloc - TR * a
        return (pltpu.make_async_copy(tl_ref.at[:, pl.ds(128 * a, 128)],
                                      vbuf.at[c, pl.ds(base_of(a), 64), :], lsem.at[0, a]),
                pltpu.make_async_copy(v_ref.at[pl.ds(TR * a, n), pl.ds(128 * a, 128)],
                                      vbuf.at[c, pl.ds(base_of(a) + 64, n), :], lsem.at[1, a]))

    def move(q, a, sem, p):
        return rc(block(q, a), block(q, a), sem, vrecv.at[a, q], (rr, p))

    def sends(a):
        return [move(c, a, vsend.at[a, n], p) for n, p in enumerate((first, second, mate))]

    def near(a):
        return [move(first, a, rsend.at[a], second), move(first, a, fsend.at[a, 0], mate),
                move(second, a, fsend.at[a, 1], mate)]

    def far(a):
        return [move(dg, a, fsend.at[a, 2], mate)]

    def arrive(a, q):
        move(q, a, vsend.at[a, 0], mate).wait_recv()

    def stage1(a):
        for cp in locals_(a):
            cp.wait()
        for cp in sends(a):
            cp.start()

    def stage2(a):
        arrive(a, first)
        arrive(a, second)
        for cp in near(a):
            cp.start()

    def stage3(a):
        arrive(a, dg)
        for cp in far(a):
            cp.start()

    def stage4(a):
        for q in others:
            arrive(a, q)

    def mycols():
        return pl.ds(pl.multiple_of(rr * rloc, rloc), rloc)

    zin = [pltpu.make_async_copy(zt_ref.at[pl.ds(16 * p, 16), mycols()], xt.at[p, r16(rr), :], zlsem.at[p])
           for p in (0, 1)]
    zcp = [rc(zt_ref.at[pl.ds(16 * p, 16), pl.ds(pl.multiple_of(zpeer(d) * rloc, rloc), rloc)],
              xt.at[p, r16(rr), :], zsend.at[p, d - 1], zrecv.at[p, d - 1], (zpeer(d), c))
           for p in (0, 1) for d in (1, 2, 3)]
    for a in range(na - 1, -1, -1):
        for cp in locals_(a):
            cp.start()
    stage1(na - 1)
    for cp in zin + zcp:
        cp.start()
    stage1(na - 2)

    lane = lax.broadcasted_iota(jnp.int32, (1, 128), 1)
    lo = lane < 64

    def deint(b, tt):
        sel = tt == 0
        out = []
        for n in range(0, len(b), 2):
            lft = jnp.where(lo, b[n], pltpu.roll(b[n + 1], 64, axis=1))
            rgt = jnp.where(lo, pltpu.roll(b[n], 64, axis=1), b[n + 1])
            out.append(jnp.where(sel, lft, rgt))
        return jnp.concatenate(out, axis=1)

    def vrows(slot, t):
        return pl.ds(pl.multiple_of(slot * rloc - TR * ((slot + 1) // 2) + t * TR, TR), TR)

    def prepare(g):
        a = na - 1 - g // 2
        tt = 1 - g % 2
        slot = lax.rem(g, 3)
        base = base_of(a)
        gpart[...] = jnp.zeros_like(gpart)

        def tile(k, _):
            t, hb = k // 2, k % 2
            src = pl.ds(pl.multiple_of(base + 64 + (t - a) * TR, 64), TR)
            v3 = split3(deint([vbuf[4 * hb + n, src, :] for n in range(4)], tt))
            o = vrows(slot, t)
            cols = pl.ds(pl.multiple_of(256 * hb, 256), 256)
            vnh[o, cols], vnm[o, cols], vnl[o, cols] = v3
            own = vbuf[c, src, :]
            own = jnp.where(tt == 0, own, pltpu.roll(own, 64, axis=1)).T[0:64, :]
            gpart[:, cols] += dot6(stack3(own), v3, 1, 0)
            return 0

        lax.fori_loop(2 * a, 2 * na, tile, 0)

    def gcopies():
        return [rc(gpart.at[r16(zpeer(d)), :], grs.at[d - 1],
                   gsend.at[d - 1], grecv.at[d - 1], (zpeer(d), c)) for d in (1, 2, 3)]

    def gmine():
        return pl.ds(pl.multiple_of(64 * c + 16 * rr, 16), 16)

    def slab(q):
        return pl.ds(pl.multiple_of(64 * q, 64), 64)

    def hcopies(gs):
        return [rc(gbuf.at[gs, gmine(), :], gbuf.at[gs, gmine(), :],
                   hsend.at[d - 1], hrecv.at[d - 1], (zpeer(d), c)) for d in (1, 2, 3)]

    def pcopies(gs):
        return [rc(gbuf.at[gs, slab(c), :], gbuf.at[gs, slab(c), :], psend.at[n], precv.at[gs, c], (rr, p))
                for n, p in enumerate((xn, yn, dg, mate))]

    def pforwards(gs):
        return [rc(gbuf.at[gs, slab(q), :], gbuf.at[gs, slab(q), :], pfsend.at[n], precv.at[gs, q], (rr, mate))
                for n, q in enumerate(same)]

    def pin(gs, q):
        return rc(gbuf.at[gs, slab(q), :], gbuf.at[gs, slab(q), :], psend.at[0], precv.at[gs, q], (rr, mate))

    def gram_start():
        for cp in gcopies():
            cp.start()

    def gram_sum(gs):
        for cp in gcopies():
            cp.wait_recv()
        gbuf[gs, gmine(), :] = (gpart[r16(rr), :] + grs[0]) + (grs[1] + grs[2])
        for cp in hcopies(gs):
            cp.start()
        for cp in gcopies():
            cp.wait_send()

    def gram_plane(gs):
        for cp in hcopies(gs):
            cp.wait()
        for cp in pcopies(gs):
            cp.start()

    def gram_forward(gs):
        for q in same:
            pin(gs, q).wait_recv()
        for cp in pforwards(gs):
            cp.start()

    def gram_finish(gs):
        for q in others:
            pin(gs, q).wait_recv()
        for cp in pcopies(gs) + pforwards(gs):
            cp.wait_send()

    lane2 = lax.broadcasted_iota(jnp.int32, (1, 256), 1) // 64

    def form_t(g_idx):
        gs = g_idx % 2
        ga = na - 1 - g_idx // 2
        gt = 1 - g_idx % 2
        head = pl.ds(pl.multiple_of(base_of(ga), 64), 64)
        z256 = jnp.zeros((64, 256), F32)

        def half(n, _):
            o = pl.ds(pl.multiple_of(256 * n, 256), 256)
            tcv = deint([vbuf[4 * n + k, head, :] for k in range(4)], gt)
            th[n] = jnp.concatenate([jnp.where(lane2 == k, tcv, 0.0) for k in range(4)], axis=0)
            g = gbuf.at[gs, o, o]
            th[3] = jnp.concatenate([jnp.where(lane2 == 1, g[0:64, :], 0.0), z256,
                                     jnp.where(lane2 == 3, g[128:192, :], 0.0), z256], axis=0)

            def na_(k, _):
                q = pl.ds(pl.multiple_of(64 * k, 64), 64)
                th[2, q, :] = dot6(stack3(th[3, q, :]), split3(th[n]), 1, 0)
                return 0

            lax.fori_loop(0, 4, na_, 0)

            def nb_(k, _):
                q = pl.ds(pl.multiple_of(64 * k, 64), 64)
                th[n, q, :] = th[n, q, :] - dot6(stack3(th[n, q, :]), split3(th[2]), 1, 0)
                return 0

            lax.fori_loop(0, 4, nb_, 0)
            tx = dot(g[0:128, 128:256], th[n, 128:256, 128:256], 1, 0)
            th[n, 0:128, 128:256] = -dot(th[n, 0:128, 0:128], tx, 1, 0)
            return 0

        lax.fori_loop(0, 2, half, 0)

        def nc_(k, _):
            q = pl.ds(pl.multiple_of(64 * k, 64), 64)
            th[2, q, :] = dot6(stack3(gbuf[gs, q, 256:512]), split3(th[1]), 1, 0)
            return 0

        lax.fori_loop(0, 4, nc_, 0)

        def nd_(k, _):
            q = pl.ds(pl.multiple_of(64 * k, 64), 64)
            th[3, q, :] = -dot6(stack3(th[0, q, :]), split3(th[2]), 1, 0)
            return 0

        lax.fori_loop(0, 4, nd_, 0)

        def put(n, _):
            src = lax.rem(3 * n, 5)
            tmh[gs, n], tmm[gs, n], tml[gs, n] = split3(th[src].T)
            return 0

        lax.fori_loop(0, 3, put, 0)

    def wcopies(p):
        return [rc(wp.at[p, r16(zpeer(d)), :], wrs.at[p, d - 1],
                   wsend.at[p, d - 1], wrecv.at[p, d - 1], (zpeer(d), c)) for d in (1, 2, 3)]

    def ycopies(p):
        return [rc(ybuf.at[p, r16(rr), :], ybuf.at[p, r16(rr), :],
                   ysend.at[p, d - 1], yrecv.at[p, d - 1], (zpeer(d), c)) for d in (1, 2, 3)]

    def w_part(i, p):
        a = na - 1 - i // 2
        slot = lax.rem(i, 3)
        wp[p] = jnp.zeros((64, 512), F32)

        def wtile(t, _):
            o = pl.ds(pl.multiple_of(t * TR, TR), TR)
            vo = vrows(slot, t)
            x3 = stack3(xt[p, :, o])
            for h in (slice(0, 256), slice(256, 512)):
                wp[p, :, h] += dot6(x3, (vnh[vo, h], vnm[vo, h], vnl[vo, h]), 1, 0)
            return 0

        lax.fori_loop(a, na, wtile, 0)
        for cp in wcopies(p):
            cp.start()

    def y_part(i, p):
        for cp in wcopies(p):
            cp.wait_recv()
        w = (wp[p, r16(rr), :] + wrs[p, 0]) + (wrs[p, 1] + wrs[p, 2])
        ts = i % 2
        wa, wb = stack3(w[:, 0:256]), stack3(w[:, 256:512])
        tb = [(tmh[ts, n], tmm[ts, n], tml[ts, n]) for n in range(3)]
        ybuf[p, r16(rr), 0:256] = dot6(wa, tb[0], 1, 0) + dot6(wb, tb[1], 1, 0)
        ybuf[p, r16(rr), 256:512] = dot6(wb, tb[2], 1, 0)
        for cp in ycopies(p):
            cp.start()
        for cp in wcopies(p):
            cp.wait_send()

    def x_part(i, p):
        a = na - 1 - i // 2
        slot = lax.rem(i, 3)
        for cp in ycopies(p):
            cp.wait_recv()
        ystk[...] = stack3(ybuf[p])

        def utile(t, _):
            o = pl.ds(pl.multiple_of(t * TR, TR), TR)
            vo = vrows(slot, t)
            xt[p, :, o] = xt[p, :, o] - dot6(ystk[...], (vnh[vo, :], vnm[vo, :], vnl[vo, :]), 1, 1)
            return 0

        lax.fori_loop(a, na, utile, 0)
        for cp in ycopies(p):
            cp.wait_send()

    stage2(na - 1)
    stage3(na - 1)
    stage4(na - 1)
    prepare(0)
    gram_start()
    gram_sum(0)
    gram_plane(0)
    if na >= 3:
        stage1(na - 3)
    prepare(1)
    gram_start()
    for cp in zin:
        cp.wait()
    for cp in zcp:
        cp.wait_recv()
    gram_forward(0)
    gram_finish(0)
    form_t(0)
    gram_sum(1)
    if na >= 2:
        stage2(na - 2)
        stage3(na - 2)

    def step(i, _):
        ns = (i + 1) % 2
        w_part(i, 0)

        @pl.when(i < nsteps - 1)
        def _():
            gram_plane(ns)

        for sa in range(na - 3, -1, -1):
            due = 2 * (na - 1 - sa) - 2

            @pl.when(i == due - 2)
            def _():
                stage2(sa)

            @pl.when(i == due - 1)
            def _():
                stage3(sa)

            if due >= 4:
                @pl.when(i == max(due - 5, 0))
                def _():
                    stage1(sa)

        @pl.when(i > 0)
        def _():
            x_part(i - 1, 1)

        w_part(i, 1)
        y_part(i, 0)

        @pl.when(i < nsteps - 1)
        def _():
            gram_forward(ns)

        for sa in range(na - 2, -1, -1):
            @pl.when(i == 2 * (na - 1 - sa) - 2)
            def _():
                stage4(sa)

        @pl.when(i < nsteps - 2)
        def _():
            prepare(i + 2)
            gram_start()

        y_part(i, 1)

        @pl.when(i < nsteps - 1)
        def _():
            gram_finish(ns)
            form_t(i + 1)

        x_part(i, 0)

        @pl.when(i < nsteps - 2)
        def _():
            gram_sum(i % 2)

        return 0

    lax.fori_loop(0, nsteps, step, 0)

    def outcopies(p):
        return [rc(xt.at[p, r16(zpeer(d)), :], out_ref.at[pl.ds(16 * p, 16), mycols()],
                   osend.at[p, d - 1], orecv.at[p, d - 1], (zpeer(d), c)) for d in (1, 2, 3)]

    oloc = [pltpu.make_async_copy(xt.at[p, r16(rr), :], out_ref.at[pl.ds(16 * p, 16), mycols()], zlsem.at[p])
            for p in (0, 1)]
    oloc[0].start()
    for cp in outcopies(0):
        cp.start()
    x_part(nsteps - 1, 1)
    oloc[1].start()
    for cp in outcopies(1):
        cp.start()
    for a in range(na - 1, -1, -1):
        for cp in sends(a) + near(a) + far(a):
            cp.wait_send()
    for cp in zcp:
        cp.wait_send()
    for p in (0, 1):
        oloc[p].wait()
        for cp in outcopies(p):
            cp.wait()


def solution(mesh):
    def body(v_loc, t_loc, z_loc):
        nt, bw = t_loc.shape[0], t_loc.shape[1]
        na = nt // 2
        rloc = v_loc.shape[0]
        tl = t_loc.transpose(1, 0, 2).reshape(bw, nt * bw)
        zt = z_loc.T
        dma = pltpu.SemaphoreType.DMA
        tot = 128 * na * (na + 1) + 64 * na
        anyspec = pl.BlockSpec(memory_space=pl.ANY)
        out = pl.pallas_call(
            functools.partial(kernel, na),
            out_shape=jax.ShapeDtypeStruct(zt.shape, F32),
            in_specs=[anyspec] * 3,
            out_specs=anyspec,
            scratch_shapes=[
                pltpu.VMEM((8, tot, 128), F32),
                pltpu.VMEM((2, 64, rloc), F32),
                pltpu.VMEM((3 * rloc - TR, 512), BF16), pltpu.VMEM((3 * rloc - TR, 512), BF16), pltpu.VMEM((3 * rloc - TR, 512), BF16),
                pltpu.VMEM((2, 3, 256, 256), BF16), pltpu.VMEM((2, 3, 256, 256), BF16), pltpu.VMEM((2, 3, 256, 256), BF16),
                pltpu.VMEM((4, 256, 256), F32),
                pltpu.VMEM((2, 64, 512), F32),
                pltpu.VMEM((2, 3, 16, 512), F32),
                pltpu.VMEM((2, 64, 512), F32),
                pltpu.VMEM((192, 512), BF16),
                pltpu.VMEM((64, 512), F32),
                pltpu.VMEM((3, 16, 512), F32),
                pltpu.VMEM((2, 512, 512), F32),
                dma((2, na)), dma((2,)),
                dma((na, 3)), dma((na, 8)), dma((na, 3)), dma((na,)),
                dma((2, 3)), dma((2, 3)), dma((2, 3)), dma((2, 3)),
                dma((2, 3)), dma((2, 3)), dma((2, 3)), dma((2, 3)),
                dma((3,)), dma((3,)), dma((3,)), dma((3,)), dma((4,)), dma((2, 8)), dma((3,)),
            ],
            compiler_params=pltpu.CompilerParams(
                collective_id=0, has_side_effects=True, vmem_limit_bytes=67043328),
        )(v_loc, tl, zt)
        return out.T

    return jax.shard_map(
        body,
        mesh=mesh,
        in_specs=(P("row", "col"), P("col", None, None), P(None, ("row", "col"))),
        out_specs=P(None, ("row", "col")),
        check_vma=False,
    )
```

```python
import functools

import jax
import jax.numpy as jnp
from jax import lax
from jax.experimental import pallas as pl
from jax.experimental.pallas import tpu as pltpu
from jax.sharding import PartitionSpec as P

F32 = jnp.float32
BF16 = jnp.bfloat16
HI = lax.Precision.HIGHEST
MESH = pl.DeviceIdType.MESH
TR = 256


def dot(a, b, ca, cb):
    return lax.dot_general(a, b, (((ca,), (cb,)), ((), ())), precision=HI, preferred_element_type=F32)


def split3(x):
    h = x.astype(BF16)
    r = x - h.astype(F32)
    m = r.astype(BF16)
    return h, m, (r - m.astype(F32)).astype(BF16)


def stack3(x):
    return jnp.concatenate(split3(x), axis=0)


def dot6(stack, parts, ca, cb):
    m = stack.shape[0] // 3
    dims = (((ca,), (cb,)), ((), ()))
    r1 = lax.dot_general(stack, parts[0], dims, preferred_element_type=F32)
    r2 = lax.dot_general(stack[0:2 * m], parts[1], dims, preferred_element_type=F32)
    r3 = lax.dot_general(stack[0:m], parts[2], dims, preferred_element_type=F32)
    return (((r1[2 * m:] + r3) + r2[m:]) + (r1[m:2 * m] + r2[0:m])) + r1[0:m]


def kernel(na, v_ref, tl_ref, zt_ref, out_ref, vbuf, xt, vnh, vnm, vnl, tmh, tmm, tml, th, wp, wrs, ybuf, ystk, gpart, grs, gbuf,
           lsem, zlsem, vsend, vrecv, fsend, rsend, zsend, zrecv, osend, orecv,
           wsend, wrecv, ysend, yrecv, gsend, grecv, hsend, hrecv, psend, precv, pfsend):
    rr = lax.axis_index("row")
    c = lax.axis_index("col")
    rloc = TR * na
    nsteps = 2 * na
    core, cx, cy = c % 2, (c // 2) % 2, c // 4
    mate = c + 1 - 2 * core
    xn = c + 2 - 4 * cx
    yn = c + 4 - 8 * cy
    dg = yn + 2 - 4 * cx
    same = (xn, yn, dg)
    others = (mate, mate + xn - c, mate + yn - c, mate + dg - c)

    def zpeer(d):
        return lax.rem(rr + d, 4)

    def r16(r):
        return pl.ds(pl.multiple_of(16 * r, 16), 16)

    barrier = pltpu.get_barrier_semaphore()
    for p in (mate, xn, yn, dg):
        pl.semaphore_signal(barrier, inc=1, device_id=(rr, p), device_id_type=MESH)
    for d in (1, 2, 3):
        pl.semaphore_signal(barrier, inc=1, device_id=(zpeer(d), c), device_id_type=MESH)
    pl.semaphore_wait(barrier, 7)

    first = xn + core * (yn - xn)
    second = yn + core * (xn - yn)

    def base_of(a):
        return 128 * (na - 1 - a) * (na - a) + 64 * (na - 1 - a)

    def block(q, a):
        return vbuf.at[q, pl.ds(base_of(a), rloc - TR * a + 64), :]

    def rc(src, dst, ss, rs, dev):
        return pltpu.make_async_remote_copy(src_ref=src, dst_ref=dst, send_sem=ss, recv_sem=rs,
                                            device_id=dev, device_id_type=MESH)

    def locals_(a):
        n = rloc - TR * a
        return (pltpu.make_async_copy(tl_ref.at[:, pl.ds(128 * a, 128)],
                                      vbuf.at[c, pl.ds(base_of(a), 64), :], lsem.at[0, a]),
                pltpu.make_async_copy(v_ref.at[pl.ds(TR * a, n), pl.ds(128 * a, 128)],
                                      vbuf.at[c, pl.ds(base_of(a) + 64, n), :], lsem.at[1, a]))

    def move(q, a, sem, p):
        return rc(block(q, a), block(q, a), sem, vrecv.at[a, q], (rr, p))

    def sends(a):
        return [move(c, a, vsend.at[a, n], p) for n, p in enumerate((first, second, mate))]

    def near(a):
        return [move(first, a, rsend.at[a], second), move(first, a, fsend.at[a, 0], mate),
                move(second, a, fsend.at[a, 1], mate)]

    def far(a):
        return [move(dg, a, fsend.at[a, 2], mate)]

    def arrive(a, q):
        move(q, a, vsend.at[a, 0], mate).wait_recv()

    def stage1(a):
        for cp in locals_(a):
            cp.wait()
        for cp in sends(a):
            cp.start()

    def stage2(a):
        arrive(a, first)
        arrive(a, second)
        for cp in near(a):
            cp.start()

    def stage3(a):
        arrive(a, dg)
        for cp in far(a):
            cp.start()

    def stage4(a):
        for q in others:
            arrive(a, q)

    def mycols():
        return pl.ds(pl.multiple_of(rr * rloc, rloc), rloc)

    zin = [pltpu.make_async_copy(zt_ref.at[pl.ds(16 * p, 16), mycols()], xt.at[p, r16(rr), :], zlsem.at[p])
           for p in (0, 1)]
    zcp = [rc(zt_ref.at[pl.ds(16 * p, 16), pl.ds(pl.multiple_of(zpeer(d) * rloc, rloc), rloc)],
              xt.at[p, r16(rr), :], zsend.at[p, d - 1], zrecv.at[p, d - 1], (zpeer(d), c))
           for p in (0, 1) for d in (1, 2, 3)]
    for a in range(na - 1, -1, -1):
        for cp in locals_(a):
            cp.start()
    stage1(na - 1)
    for cp in zin + zcp:
        cp.start()
    stage1(na - 2)

    lane = lax.broadcasted_iota(jnp.int32, (1, 128), 1)
    lo = lane < 64

    def deint(b, tt):
        sel = tt == 0
        out = []
        for n in range(0, len(b), 2):
            lft = jnp.where(lo, b[n], pltpu.roll(b[n + 1], 64, axis=1))
            rgt = jnp.where(lo, pltpu.roll(b[n], 64, axis=1), b[n + 1])
            out.append(jnp.where(sel, lft, rgt))
        return jnp.concatenate(out, axis=1)

    def vrows(slot, t):
        return pl.ds(pl.multiple_of(slot * rloc - TR * ((slot + 1) // 2) + t * TR, TR), TR)

    def prepare(g):
        a = na - 1 - g // 2
        tt = 1 - g % 2
        slot = lax.rem(g, 3)
        base = base_of(a)
        gpart[...] = jnp.zeros_like(gpart)

        def tile(k, _):
            t, hb = k // 2, k % 2
            src = pl.ds(pl.multiple_of(base + 64 + (t - a) * TR, 64), TR)
            v3 = split3(deint([vbuf[4 * hb + n, src, :] for n in range(4)], tt))
            o = vrows(slot, t)
            cols = pl.ds(pl.multiple_of(256 * hb, 256), 256)
            vnh[o, cols], vnm[o, cols], vnl[o, cols] = v3
            own = vbuf[c, src, :]
            own = jnp.where(tt == 0, own, pltpu.roll(own, 64, axis=1)).T[0:64, :]
            gpart[:, cols] += dot6(stack3(own), v3, 1, 0)
            return 0

        lax.fori_loop(2 * a, 2 * na, tile, 0)

    def gcopies():
        return [rc(gpart.at[r16(zpeer(d)), :], grs.at[d - 1],
                   gsend.at[d - 1], grecv.at[d - 1], (zpeer(d), c)) for d in (1, 2, 3)]

    def gmine():
        return pl.ds(pl.multiple_of(64 * c + 16 * rr, 16), 16)

    def slab(q):
        return pl.ds(pl.multiple_of(64 * q, 64), 64)

    def hcopies(gs):
        return [rc(gbuf.at[gs, gmine(), :], gbuf.at[gs, gmine(), :],
                   hsend.at[d - 1], hrecv.at[d - 1], (zpeer(d), c)) for d in (1, 2, 3)]

    def pcopies(gs):
        return [rc(gbuf.at[gs, slab(c), :], gbuf.at[gs, slab(c), :], psend.at[n], precv.at[gs, c], (rr, p))
                for n, p in enumerate((xn, yn, dg, mate))]

    def pforwards(gs):
        return [rc(gbuf.at[gs, slab(q), :], gbuf.at[gs, slab(q), :], pfsend.at[n], precv.at[gs, q], (rr, mate))
                for n, q in enumerate(same)]

    def pin(gs, q):
        return rc(gbuf.at[gs, slab(q), :], gbuf.at[gs, slab(q), :], psend.at[0], precv.at[gs, q], (rr, mate))

    def gram_start():
        for cp in gcopies():
            cp.start()

    def gram_sum(gs):
        for cp in gcopies():
            cp.wait_recv()
        gbuf[gs, gmine(), :] = (gpart[r16(rr), :] + grs[0]) + (grs[1] + grs[2])
        for cp in hcopies(gs):
            cp.start()
        for cp in gcopies():
            cp.wait_send()

    def gram_plane(gs):
        for cp in hcopies(gs):
            cp.wait()
        for cp in pcopies(gs):
            cp.start()

    def gram_forward(gs):
        for q in same:
            pin(gs, q).wait_recv()
        for cp in pforwards(gs):
            cp.start()

    def gram_finish(gs):
        for q in others:
            pin(gs, q).wait_recv()
        for cp in pcopies(gs) + pforwards(gs):
            cp.wait_send()

    lane2 = lax.broadcasted_iota(jnp.int32, (1, 256), 1) // 64

    def form_t(g_idx):
        gs = g_idx % 2
        ga = na - 1 - g_idx // 2
        gt = 1 - g_idx % 2
        head = pl.ds(pl.multiple_of(base_of(ga), 64), 64)
        z256 = jnp.zeros((64, 256), F32)

        def half(n, _):
            o = pl.ds(pl.multiple_of(256 * n, 256), 256)
            tcv = deint([vbuf[4 * n + k, head, :] for k in range(4)], gt)
            th[n] = jnp.concatenate([jnp.where(lane2 == k, tcv, 0.0) for k in range(4)], axis=0)
            g = gbuf.at[gs, o, o]
            th[3] = jnp.concatenate([jnp.where(lane2 == 1, g[0:64, :], 0.0), z256,
                                     jnp.where(lane2 == 3, g[128:192, :], 0.0), z256], axis=0)

            def na_(k, _):
                q = pl.ds(pl.multiple_of(64 * k, 64), 64)
                th[2, q, :] = dot6(stack3(th[3, q, :]), split3(th[n]), 1, 0)
                return 0

            lax.fori_loop(0, 4, na_, 0)

            def nb_(k, _):
                q = pl.ds(pl.multiple_of(64 * k, 64), 64)
                th[n, q, :] = th[n, q, :] - dot6(stack3(th[n, q, :]), split3(th[2]), 1, 0)
                return 0

            lax.fori_loop(0, 4, nb_, 0)
            tx = dot(g[0:128, 128:256], th[n, 128:256, 128:256], 1, 0)
            th[n, 0:128, 128:256] = -dot(th[n, 0:128, 0:128], tx, 1, 0)
            return 0

        lax.fori_loop(0, 2, half, 0)

        def nc_(k, _):
            q = pl.ds(pl.multiple_of(64 * k, 64), 64)
            th[2, q, :] = dot6(stack3(gbuf[gs, q, 256:512]), split3(th[1]), 1, 0)
            return 0

        lax.fori_loop(0, 4, nc_, 0)

        def nd_(k, _):
            q = pl.ds(pl.multiple_of(64 * k, 64), 64)
            th[3, q, :] = -dot6(stack3(th[0, q, :]), split3(th[2]), 1, 0)
            return 0

        lax.fori_loop(0, 4, nd_, 0)

        def put(n, _):
            src = lax.rem(3 * n, 5)
            tmh[gs, n], tmm[gs, n], tml[gs, n] = split3(th[src].T)
            return 0

        lax.fori_loop(0, 3, put, 0)

    def wcopies(p):
        return [rc(wp.at[p, r16(zpeer(d)), :], wrs.at[p, d - 1],
                   wsend.at[p, d - 1], wrecv.at[p, d - 1], (zpeer(d), c)) for d in (1, 2, 3)]

    def ycopies(p):
        return [rc(ybuf.at[p, r16(rr), :], ybuf.at[p, r16(rr), :],
                   ysend.at[p, d - 1], yrecv.at[p, d - 1], (zpeer(d), c)) for d in (1, 2, 3)]

    def w_part(i, p):
        a = na - 1 - i // 2
        slot = lax.rem(i, 3)
        wp[p] = jnp.zeros((64, 512), F32)

        def wtile(t, _):
            o = pl.ds(pl.multiple_of(t * TR, TR), TR)
            vo = vrows(slot, t)
            x3 = stack3(xt[p, :, o])
            for h in (slice(0, 256), slice(256, 512)):
                wp[p, :, h] += dot6(x3, (vnh[vo, h], vnm[vo, h], vnl[vo, h]), 1, 0)
            return 0

        lax.fori_loop(a, na, wtile, 0)
        for cp in wcopies(p):
            cp.start()

    def y_part(i, p):
        for cp in wcopies(p):
            cp.wait_recv()
        w = (wp[p, r16(rr), :] + wrs[p, 0]) + (wrs[p, 1] + wrs[p, 2])
        ts = i % 2
        wa, wb = stack3(w[:, 0:256]), stack3(w[:, 256:512])
        tb = [(tmh[ts, n], tmm[ts, n], tml[ts, n]) for n in range(3)]
        ybuf[p, r16(rr), 0:256] = dot6(wa, tb[0], 1, 0) + dot6(wb, tb[1], 1, 0)
        ybuf[p, r16(rr), 256:512] = dot6(wb, tb[2], 1, 0)
        for cp in ycopies(p):
            cp.start()
        for cp in wcopies(p):
            cp.wait_send()

    def x_part(i, p):
        a = na - 1 - i // 2
        slot = lax.rem(i, 3)
        for cp in ycopies(p):
            cp.wait_recv()
        ystk[...] = stack3(ybuf[p])

        def utile(t, _):
            o = pl.ds(pl.multiple_of(t * TR, TR), TR)
            vo = vrows(slot, t)
            xt[p, :, o] = xt[p, :, o] - dot6(ystk[...], (vnh[vo, :], vnm[vo, :], vnl[vo, :]), 1, 1)
            return 0

        lax.fori_loop(a, na, utile, 0)
        for cp in ycopies(p):
            cp.wait_send()

    stage2(na - 1)
    stage3(na - 1)
    stage4(na - 1)
    prepare(0)
    gram_start()
    gram_sum(0)
    gram_plane(0)
    for a in range(na - 3, max(na - 5, -1), -1):
        stage1(a)
    prepare(1)
    gram_start()
    for cp in zin:
        cp.wait()
    for cp in zcp:
        cp.wait_recv()
    gram_forward(0)
    gram_finish(0)
    form_t(0)
    gram_sum(1)
    if na >= 2:
        stage2(na - 2)
        stage3(na - 2)

    def step(i, _):
        ns = (i + 1) % 2
        w_part(i, 0)

        @pl.when(i < nsteps - 1)
        def _():
            gram_plane(ns)

        @pl.when(i > 0)
        def _():
            x_part(i - 1, 1)

        w_part(i, 1)
        y_part(i, 0)

        @pl.when(i < nsteps - 1)
        def _():
            gram_forward(ns)

        for sa in range(na - 3, -1, -1):
            due = 2 * (na - 1 - sa) - 2

            @pl.when(i == due - 2)
            def _():
                stage2(sa)

            @pl.when(i == due - 1)
            def _():
                stage3(sa)

            if due >= 6:
                @pl.when(i == due - 6)
                def _():
                    stage1(sa)

        for sa in range(na - 2, -1, -1):
            @pl.when(i == 2 * (na - 1 - sa) - 2)
            def _():
                stage4(sa)

        @pl.when(i < nsteps - 2)
        def _():
            prepare(i + 2)
            gram_start()

        y_part(i, 1)

        @pl.when(i < nsteps - 1)
        def _():
            gram_finish(ns)
            form_t(i + 1)

        x_part(i, 0)

        @pl.when(i < nsteps - 2)
        def _():
            gram_sum(i % 2)

        return 0

    lax.fori_loop(0, nsteps, step, 0)

    def outcopies(p):
        return [rc(xt.at[p, r16(zpeer(d)), :], out_ref.at[pl.ds(16 * p, 16), mycols()],
                   osend.at[p, d - 1], orecv.at[p, d - 1], (zpeer(d), c)) for d in (1, 2, 3)]

    oloc = [pltpu.make_async_copy(xt.at[p, r16(rr), :], out_ref.at[pl.ds(16 * p, 16), mycols()], zlsem.at[p])
            for p in (0, 1)]
    oloc[0].start()
    for cp in outcopies(0):
        cp.start()
    x_part(nsteps - 1, 1)
    oloc[1].start()
    for cp in outcopies(1):
        cp.start()
    for a in range(na - 1, -1, -1):
        for cp in sends(a) + near(a) + far(a):
            cp.wait_send()
    for cp in zcp:
        cp.wait_send()
    for p in (0, 1):
        oloc[p].wait()
        for cp in outcopies(p):
            cp.wait()


def solution(mesh):
    def body(v_loc, t_loc, z_loc):
        nt, bw = t_loc.shape[0], t_loc.shape[1]
        na = nt // 2
        rloc = v_loc.shape[0]
        tl = t_loc.transpose(1, 0, 2).reshape(bw, nt * bw)
        zt = z_loc.T
        dma = pltpu.SemaphoreType.DMA
        tot = 128 * na * (na + 1) + 64 * na
        anyspec = pl.BlockSpec(memory_space=pl.ANY)
        out = pl.pallas_call(
            functools.partial(kernel, na),
            out_shape=jax.ShapeDtypeStruct(zt.shape, F32),
            in_specs=[anyspec] * 3,
            out_specs=anyspec,
            scratch_shapes=[
                pltpu.VMEM((8, tot, 128), F32),
                pltpu.VMEM((2, 64, rloc), F32),
                pltpu.VMEM((3 * rloc - TR, 512), BF16), pltpu.VMEM((3 * rloc - TR, 512), BF16), pltpu.VMEM((3 * rloc - TR, 512), BF16),
                pltpu.VMEM((2, 3, 256, 256), BF16), pltpu.VMEM((2, 3, 256, 256), BF16), pltpu.VMEM((2, 3, 256, 256), BF16),
                pltpu.VMEM((4, 256, 256), F32),
                pltpu.VMEM((2, 64, 512), F32),
                pltpu.VMEM((2, 3, 16, 512), F32),
                pltpu.VMEM((2, 64, 512), F32),
                pltpu.VMEM((192, 512), BF16),
                pltpu.VMEM((64, 512), F32),
                pltpu.VMEM((3, 16, 512), F32),
                pltpu.VMEM((2, 512, 512), F32),
                dma((2, na)), dma((2,)),
                dma((na, 3)), dma((na, 8)), dma((na, 3)), dma((na,)),
                dma((2, 3)), dma((2, 3)), dma((2, 3)), dma((2, 3)),
                dma((2, 3)), dma((2, 3)), dma((2, 3)), dma((2, 3)),
                dma((3,)), dma((3,)), dma((3,)), dma((3,)), dma((4,)), dma((2, 8)), dma((3,)),
            ],
            compiler_params=pltpu.CompilerParams(
                collective_id=0, has_side_effects=True, vmem_limit_bytes=67043328),
        )(v_loc, tl, zt)
        return out.T

    return jax.shard_map(
        body,
        mesh=mesh,
        in_specs=(P("row", "col"), P("col", None, None), P(None, ("row", "col"))),
        out_specs=P(None, ("row", "col")),
        check_vma=False,
    )
```
